32 devices in a mesh: tok: 8 (over y, x, core), col: 4 (over z).
Axes of the slice: x: 2, y: 2, z: 4, core: 2. Of those that a mesh axis runs over, the one named last changes fastest.
Arguments:
- acts_a: bfloat16 [8192, 3584], P('tok', 'col'), may hold values from -6 to 6
- acts_b: bfloat16 [8192, 4096], P('tok', 'col'), may hold values from -6 to 6
- whiten_a: bfloat16 [3584, 3584], P(None, 'col'), may hold values from -0.09375 to 0.09375
- whiten_b: bfloat16 [4096, 4096], P(None, 'col'), may hold values from -0.09375 to 0.09375
Outputs:
- cross: float32 [3584, 4096], P('col', 'tok')
The draws below stay inside these ranges and needn't reach their ends.
All inputs are finite; a program needn't handle non-finite values.
Results may differ from the reference program's by a relative error of at most 0.0041.
Values may be sent and summed in bfloat16 or wider, within the bound.
A program may use at most 128 MiB of HBM per device.

```python
import jax
import jax.numpy as jnp
from jax import lax

DA = 3584
DB = 4096
TOKENS = 8192


def shard_levels(own_key, shape, pieces, low, top_value):
    def one(dim, shards_of):
        heights = jax.random.uniform(jax.random.fold_in(jax.random.fold_in(own_key, 6), dim), (shards_of,), jnp.float32, low / len(pieces), top_value / len(pieces))
        return jnp.repeat(jnp.exp(heights), shape[dim] // shards_of).reshape((-1,) + (1,) * (len(shape) - dim - 1))

    loudness = one(*pieces[0])
    for cut in pieces[1:]:
        loudness = loudness * one(*cut)
    return loudness


def bell_draw(key, shape, spread, bound, shards=(), held_as=jnp.bfloat16):
    drawn = jax.random.normal(key, shape, jnp.float32) * spread
    if len(shards) > 0:
        drawn = shard_levels(key, shape, shards, -0.22, 0.18) * drawn
    return jnp.clip(drawn, min=-bound, max=bound).astype(held_as)


def setup_inputs(seed: int = 0) -> dict:
    streams_of = jax.random.split(jax.random.key(seed), 5)
    acts_a = bell_draw(streams_of[0], (TOKENS, DA), 1.0, 6.0, ((0, 8), (1, 4)))
    acts_b = bell_draw(streams_of[1], (TOKENS, DB), 1.0, 6.0, ((0, 8), (1, 4)))
    whiten_a = bell_draw(streams_of[2], (DA, DA), DA ** -0.5, 0.09375, ((1, 4),))
    whiten_b = bell_draw(streams_of[3], (DB, DB), DB ** -0.5, 0.09375, ((1, 4),))
    return {"acts_a": acts_a, "acts_b": acts_b, "whiten_a": whiten_a, "whiten_b": whiten_b}


def reference(acts_a, acts_b, whiten_a, whiten_b):
    white_a = jnp.dot(acts_a, whiten_a, preferred_element_type=jnp.float32).astype(jnp.bfloat16)
    white_b = jnp.dot(acts_b, whiten_b, preferred_element_type=jnp.float32).astype(jnp.bfloat16)
    summed = lax.dot_general(white_a, white_b, (((0,), (0,)), ((), ())), preferred_element_type=jnp.float32)
    scale = 1.0 / jnp.sqrt(jnp.float32(TOKENS))
    return summed * scale
```

```python
import functools

import jax
import jax.numpy as jnp
from jax import lax
from jax.experimental import pallas as pl
from jax.experimental.pallas import tpu as pltpu
from jax.sharding import PartitionSpec as P

LANES = 128
SHARES = (5, 2)


def dot_tn(x, y):
    return lax.dot_general(x, y, (((0,), (0,)), ((), ())), preferred_element_type=jnp.float32)


def swap(x, step):
    return lax.ppermute(x, "tok", [(i, i ^ step) for i in range(lax.axis_size("tok"))])


def sum_tokens(part):
    size = lax.axis_size("tok")
    count = size.bit_length() - 1
    me = lax.axis_index("tok")
    rows, cols = part.shape
    done = []
    for flip in range(2):
        half = part[:, flip * (cols // 2):(flip + 1) * (cols // 2)]
        half = half.reshape((2,) * count + (rows // size, cols // 2))
        left = list(range(count - 1, -1, -1))
        for bit in [0] + list(range(1, count))[:: -1 if flip else 1]:
            axis = left.index(bit)
            mine = (me >> bit) & 1
            keep = lax.dynamic_index_in_dim(half, mine, axis, keepdims=False)
            send = lax.dynamic_index_in_dim(half, 1 - mine, axis, keepdims=False)
            half = keep + swap(send, 1 << bit)
            left.remove(bit)
        done.append(half.astype(jnp.bfloat16))
    return jnp.concatenate(done, axis=1)


def line_gather(x):
    n = lax.axis_size("col")
    z = lax.axis_index("col")
    rows, w = x.shape
    ups, downs = [x], [x]
    for s in range(1, n):
        ups.append(lax.ppermute(ups[-1], "col", [(i, i + 1) for i in range(s - 1, n - 1)]))
        downs.append(lax.ppermute(downs[-1], "col", [(i, i - 1) for i in range(1, n - s + 1)]))
    out = lax.dynamic_update_slice_in_dim(jnp.zeros((rows, n * w), x.dtype), x, z * w, 1)
    for s in range(1, n):
        block = jnp.where(z >= s, ups[s], downs[n - s])
        out = lax.dynamic_update_slice_in_dim(out, block, ((z + n - s) % n) * w, 1)
    return out


def chunks(width):
    if width % (LANES * sum(SHARES)):
        return [(0, width)]
    unit, at, out = width // sum(SHARES), 0, []
    for share in SHARES:
        out.append((at, share * unit))
        at += share * unit
    return out


def body(acts_a, acts_b, whiten_a, whiten_b):
    n, m = lax.axis_size("col"), lax.axis_size("tok")
    tokens, width = acts_a.shape

    parts = chunks(width)
    gathered = [lax.all_gather(acts_a[:, at:at + w], "col", axis=1, tiled=True) for at, w in parts]
    covs, right = [], acts_b
    for g in gathered:
        cov = sum_tokens(dot_tn(g, right))
        cov, right = lax.optimization_barrier((cov, right))
        covs.append(cov)
    covs = [line_gather(c) for c in covs]
    whiten_b, _ = lax.optimization_barrier((whiten_b, cov))
    halves = [jnp.dot(c, whiten_b, preferred_element_type=jnp.float32).astype(jnp.bfloat16) for c in covs]
    halves = [lax.all_gather(h, "col", axis=1, tiled=True) for h in halves]

    total = None
    for (at, w), half in zip(parts, halves):
        half = lax.all_to_all(half, "tok", split_axis=1, concat_axis=0, tiled=True)
        weights = whiten_a.reshape(n, width, -1)[:, at:at + w].reshape(n * w, -1)
        term = dot_tn(weights, half)
        total = term if total is None else total + term
    scale = 1.0 / jnp.sqrt(jnp.float32(tokens * m))
    return total * scale


def eligible(mesh, acts_a, acts_b):
    n, m = mesh.shape["col"], mesh.shape["tok"]
    width, depth = acts_a.shape[1] // n, acts_b.shape[1] // n
    rows = acts_a.shape[0] // m
    return n == 4 and m == 2 * n and rows % LANES == 0 and width % LANES == 0 and depth % (2 * LANES) == 0


def remote(src, dst, send, recv, z, t):
    return pltpu.make_async_remote_copy(
        src_ref=src, dst_ref=dst, send_sem=send, recv_sem=recv,
        device_id={"tok": t, "col": z}, device_id_type=pl.DeviceIdType.MESH)


def kernel(a_hbm, b_hbm, wa_hbm, wb_hbm, out, raw, at, bl, own, xs, xr, rs, rr, keep, cs, cr, wb, wat, stage, hb, hc,
           raw_sem, b_sem, bin_sem, wb_sem, st_sem, as_sem, ar_sem, xs_sem, xr_sem, rs_sem, rr_sem, cs_sem, cr_sem,
           hs_sem, hr_sem, ts_sem, tr_sem):
    K, n, _, T = at.shape
    V = bl.shape[2]
    W = wa_hbm.shape[1]
    H = V // 2
    half = LANES // 2
    t, z = lax.axis_index("tok"), lax.axis_index("col")
    g, c = t // 2, t % 2
    sib = t + 1 - 2 * c
    inner = (z == 1) | (z == 2)
    edge = z // 2 * 3
    mate = 3 - z
    far = 3 - edge
    hub = 1 + z // 3
    v = 2 * (z - 1) + c
    flips = range(1, n)

    def flip(x, d):
        lo, hi = x % 2, x // 2
        return (lo + d % 2) % 2 + 2 * ((hi + d // 2) % 2)

    def flip8(x, d):
        return (x % 2 + d % 2) % 2 + 2 * flip(x // 2, d // 2)

    def load_raw(j):
        return pltpu.make_async_copy(a_hbm.at[:, pl.ds(pl.multiple_of(j * LANES, LANES), LANES)], raw.at[j % 2], raw_sem.at[j % 2])

    def load_stage(q):
        rows = q % n * W + q // n * LANES
        return pltpu.make_async_copy(wa_hbm.at[pl.ds(pl.multiple_of(rows, LANES), LANES), :], stage.at[q % 2], st_sem.at[q % 2])

    own_b = pltpu.make_async_copy(b_hbm, bl.at[2 - z], b_sem)
    load_wb = pltpu.make_async_copy(wb_hbm, wb, wb_sem)

    def up_a(j):
        return remote(at.at[j, z], at.at[j, z], as_sem.at[0, j], ar_sem.at[z, j], hub, t)

    def across_a(j):
        return remote(at.at[j, z], at.at[j, z], as_sem.at[0, j], ar_sem.at[z, j], mate, t)

    def pass_a(j):
        return remote(at.at[j, edge], at.at[j, edge], as_sem.at[1, j], ar_sem.at[edge, j], mate, t)

    def got_a(j, src):
        return remote(at.at[j, src], at.at[j, src], as_sem.at[0, j], ar_sem.at[src, j], mate, t)

    up_b = remote(b_hbm, bl.at[hub - 1], b_sem, bin_sem, hub, t)
    got_b = remote(b_hbm, bl.at[z - 1], b_sem, bin_sem, mate, t)

    def swap_x(j):
        return remote(xs, xr.at[j % 2], xs_sem, xr_sem.at[j % 2], z, sib)

    def send_r(j, d):
        s = flip(g, d)
        return remote(rs.at[j % 2, s], rr.at[j, d - 1], rs_sem.at[j % 2, d - 1], rr_sem.at[j, d - 1], z, 2 * s + c)

    def send_c(j):
        moves = [remote(cs.at[j, 1 - c], cr.at[j, v], cs_sem.at[j, 0], cr_sem.at[j, v], z, sib)]
        for core in range(2):
            moves.append(remote(cs.at[j, core], cr.at[j, v], cs_sem.at[j, 1 + core], cr_sem.at[j, v], mate, 2 * g + core))
            moves.append(remote(cs.at[j, core], cr.at[j, v], cs_sem.at[j, 3 + core], cr_sem.at[j, v], edge, 2 * g + core))
        return moves

    def got_c(j, src):
        return remote(cs.at[j, 0], cr.at[j, src], cs_sem.at[j, 0], cr_sem.at[j, src], mate, t)

    def pass_c(j, core):
        src = 2 * (mate - 1) + core
        return remote(cr.at[j, src], cr.at[j, src], cs_sem.at[j, 5 + core], cr_sem.at[j, src], edge, t)

    def move_h(j, src, slot, to):
        return remote(hb.at[j, src], hb.at[j, src], hs_sem.at[j, slot], hr_sem.at[j, src], to, t)

    def send_t(j, d):
        peer = flip8(t, d)
        return remote(hb.at[j, peer // 2, peer % 2], hc.at[j, t], ts_sem.at[j, d - 1], tr_sem.at[j, d - 1], z, peer)

    load_raw(0).start()
    load_wb.start()
    load_stage(0).start()

    @pl.when(inner)
    def _():
        own_b.start()

    barrier = pltpu.get_barrier_semaphore()

    def greet(to, who):
        pl.semaphore_signal(barrier, inc=1, device_id={"tok": who, "col": to}, device_id_type=pl.DeviceIdType.MESH)

    for d in range(1, 2 * n):
        greet(z, flip8(t, d))

    @pl.when(inner)
    def _():
        for core in range(2):
            greet(mate, 2 * g + core)
            greet(edge, 2 * g + core)
        pl.semaphore_wait(barrier, 2 * n - 1 + 4)

    @pl.when(jnp.logical_not(inner))
    def _():
        for core in range(2):
            greet(hub, 2 * g + core)
        pl.semaphore_wait(barrier, 2 * n - 1 + 2)

    def post_a(j):
        @pl.when(inner)
        def _():
            across_a(j).start()

        @pl.when(jnp.logical_not(inner))
        def _():
            up_a(j).start()

            @pl.when(j == 0)
            def _():
                up_b.start()

    def turn_a(j, _):
        @pl.when(j + 1 < K)
        def _():
            load_raw(j + 1).start()

        load_raw(j).wait()
        at[j, z] = raw[j % 2].T

        @pl.when(j > 0)
        def _():
            post_a(j - 1)
        return 0

    lax.fori_loop(0, K, turn_a, 0)
    out[...] = jnp.zeros_like(out)
    post_a(K - 1)

    def turn_w(j, _):
        for s in range(n):
            q = j * n + s

            @pl.when(q + 1 < K * n)
            def _():
                load_stage(q + 1).start()

            load_stage(q).wait()
            wat[j, :, s * LANES:(s + 1) * LANES] = stage[q % 2].T
        return 0

    lax.fori_loop(0, K, turn_w, 0)

    def relay_a(j):
        got_a(j, edge).wait_recv()
        pass_a(j).start()

    @pl.when(inner)
    def _():
        relay_a(0)
        own_b.wait()
        got_b.wait_recv()

    load_wb.wait()
    tile = min(2 * LANES, H)

    def form(j):
        got_a(j, mate).wait_recv()
        got_a(j, far).wait_recv()

        @pl.when(j > 0)
        def _():
            swap_x(j).wait_send()

        for dst, slot in ((xs, 1 - c), (own, c)):
            def step(k, _, dst=dst, slot=slot):
                cols = pl.ds(pl.multiple_of(k * tile, tile), tile)
                part = jnp.dot(at[j].reshape(n * LANES, T), bl[slot, :, cols], preferred_element_type=jnp.float32)
                dst[:, :, cols] = part.reshape(n, LANES, tile)
                return 0

            lax.fori_loop(0, V // tile, step, 0)
            if dst is own:
                swap_x(j).start()

    def split(j):
        swap_x(j).wait_recv()

        @pl.when(j > 1)
        def _():
            for d in flips:
                send_r(j, d).wait_send()

        def step(s, _):
            total = own[s] + xr[j % 2, s]

            @pl.when(s == g)
            def _():
                keep[j % 2] = total

            rs[j % 2, s] = total.astype(rs.dtype)
            return 0

        lax.fori_loop(0, n, step, 0)
        for d in flips:
            send_r(j, d).start()

    def gather_c(j):
        for d in flips:
            send_r(j, d).wait_recv()
        total = keep[j % 2]
        for d in flips:
            total = total + rr[j, d - 1].astype(jnp.float32)
        total = total.astype(cs.dtype)
        cs[j] = total.reshape(2, half, V)
        cr[j, v] = cs[j, c]
        for move in send_c(j):
            move.start()

    def form_h(j):
        @pl.when(inner)
        def _():
            for core in range(2):
                got_c(j, 2 * (mate - 1) + core).wait_recv()
                pass_c(j, core).start()
            got_c(j, 2 * (z - 1) + 1 - c).wait_recv()

        @pl.when(jnp.logical_not(inner))
        def _():
            for src in range(n):
                got_c(j, src).wait_recv()

        for h in range(2):
            def step(k, _, h=h):
                cols = pl.ds(pl.multiple_of(h * H + k * tile, tile), tile)
                total = jnp.zeros((half, tile), jnp.float32)
                for src in range(n):
                    total += jnp.dot(cr[j, src], wb[src * V:(src + 1) * V, cols], preferred_element_type=jnp.float32)
                hb[j, z, h, :, pl.ds(pl.multiple_of(k * tile, tile), tile)] = total.astype(hb.dtype)
                return 0

            lax.fori_loop(0, H // tile, step, 0)

        @pl.when(inner)
        def _():
            move_h(j, z, 0, mate).start()
            move_h(j, z, 1, edge).start()

        @pl.when(jnp.logical_not(inner))
        def _():
            move_h(j, z, 0, hub).start()

    def spread_h(j):
        @pl.when(inner)
        def _():
            move_h(j, edge, 2, mate).wait_recv()
            move_h(j, edge, 2, mate).start()
            move_h(j, mate, 3, edge).wait_recv()
            move_h(j, mate, 3, edge).start()
            move_h(j, far, 4, edge).wait_recv()
            move_h(j, far, 4, edge).start()

        @pl.when(jnp.logical_not(inner))
        def _():
            for d in flips:
                move_h(j, flip(z, d), 0, hub).wait_recv()

        for d in range(1, 2 * n):
            send_t(j, d).start()
        hc[j, t] = hb[j, g, c]

    def gain(j):
        for d in range(1, 2 * n):
            send_t(j, d).wait_recv()

        def step(k, _):
            cols = pl.ds(pl.multiple_of(k * tile, tile), tile)
            out[:, cols] += jnp.dot(wat[j], hc[j, :, :, cols].reshape(n * LANES, tile), preferred_element_type=jnp.float32)
            return 0

        lax.fori_loop(0, H // tile, step, 0)

    def at_step(i, lag, work, only=None):
        live = (i >= lag) & (i < K + lag)
        if only is not None:
            live = live & only
        pl.when(live)(lambda: work(i - lag))

    def turn(i, _):
        at_step(i, -1, relay_a, inner & (i + 1 < K))
        at_step(i, 0, form, inner)
        at_step(i, 1, gather_c, inner)
        at_step(i, 0, split, inner)
        at_step(i, 2, form_h)
        at_step(i, 3, spread_h)
        at_step(i, 4, gain)
        return 0

    lax.fori_loop(0, K + 4, turn, 0)

    @pl.when(inner)
    def _():
        swap_x(0).wait_send()
        for j in range(max(K - 2, 0), K):
            for d in flips:
                send_r(j, d).wait_send()

    @pl.when(jnp.logical_not(inner))
    def _():
        up_b.wait_send()

    def drain(j, _):
        @pl.when(inner)
        def _():
            across_a(j).wait_send()
            pass_a(j).wait_send()
            for move in send_c(j):
                move.wait_send()
            for core in range(2):
                pass_c(j, core).wait_send()
            move_h(j, z, 0, mate).wait_send()
            move_h(j, z, 1, edge).wait_send()
            move_h(j, edge, 2, mate).wait_send()
            move_h(j, mate, 3, edge).wait_send()
            move_h(j, far, 4, edge).wait_send()

        @pl.when(jnp.logical_not(inner))
        def _():
            up_a(j).wait_send()
            move_h(j, z, 0, hub).wait_send()

        for d in range(1, 2 * n):
            send_t(j, d).wait_send()
        return 0

    lax.fori_loop(0, K, drain, 0)


def fused(mesh, acts_a, acts_b, whiten_a, whiten_b):
    n, m = lax.axis_size("col"), lax.axis_size("tok")
    T, W = acts_a.shape
    V = acts_b.shape[1]
    K = W // LANES
    bf, f32 = jnp.bfloat16, jnp.float32
    half = LANES // 2
    dma = pltpu.SemaphoreType.DMA
    flops = 2 * (n * W * T * 2 * V + K * half * n * V * V + n * W * W * V // 2)
    total = pl.pallas_call(
        kernel,
        out_shape=jax.ShapeDtypeStruct((W, V // 2), f32),
        in_specs=[pl.BlockSpec(memory_space=pl.ANY)] * 4,
        out_specs=pl.BlockSpec(memory_space=pltpu.VMEM),
        scratch_shapes=[
            pltpu.VMEM((2, T, LANES), bf),
            pltpu.VMEM((K, n, LANES, T), bf),
            pltpu.VMEM((2, T, V), bf),
            pltpu.VMEM((n, LANES, V), f32),
            pltpu.VMEM((n, LANES, V), f32),
            pltpu.VMEM((2, n, LANES, V), f32),
            pltpu.VMEM((2, n, LANES, V), bf),
            pltpu.VMEM((K, n - 1, LANES, V), bf),
            pltpu.VMEM((2, LANES, V), f32),
            pltpu.VMEM((K, 2, half, V), bf),
            pltpu.VMEM((K, n, half, V), bf),
            pltpu.VMEM((n * V, V), bf),
            pltpu.VMEM((K, W, n * LANES), bf),
            pltpu.VMEM((2, LANES, W), bf),
            pltpu.VMEM((K, n, 2, half, V // 2), bf),
            pltpu.VMEM((K, m, half, V // 2), bf),
            dma((2,)), dma, dma, dma, dma((2,)),
            dma((2, K)), dma((n, K)), dma, dma((2,)), dma((2, n - 1)), dma((K, n - 1)), dma((K, 7)), dma((K, n)),
            dma((K, 5)), dma((K, n)), dma((K, m - 1)), dma((K, m - 1)),
        ],
        compiler_params=pltpu.CompilerParams(collective_id=0, has_side_effects=True, vmem_limit_bytes=67_000_000),
        cost_estimate=pl.CostEstimate(flops=flops, bytes_accessed=2 * (T * (W + V) + n * (W * W + V * V)), transcendentals=0),
    )(acts_a, acts_b, whiten_a, whiten_b)
    return total * (1.0 / jnp.sqrt(jnp.float32(T * m)))


def solution(mesh):
    placed = (P("tok", "col"), P("tok", "col"), P(None, "col"), P(None, "col"))

    def whole(acts_a, acts_b, whiten_a, whiten_b):
        form = functools.partial(fused, mesh) if eligible(mesh, acts_a, acts_b) else body
        return jax.shard_map(form, mesh=mesh, in_specs=placed, out_specs=P("col", "tok"), check_vma=False)(
            acts_a, acts_b, whiten_a, whiten_b)

    return whole
```

```python
import functools

import jax
import jax.numpy as jnp
from jax import lax
from jax.experimental import pallas as pl
from jax.experimental.pallas import tpu as pltpu
from jax.sharding import PartitionSpec as P

LANES = 128
SHARES = (5, 2)


def dot_tn(x, y):
    return lax.dot_general(x, y, (((0,), (0,)), ((), ())), preferred_element_type=jnp.float32)


def swap(x, step):
    return lax.ppermute(x, "tok", [(i, i ^ step) for i in range(lax.axis_size("tok"))])


def sum_tokens(part):
    size = lax.axis_size("tok")
    count = size.bit_length() - 1
    me = lax.axis_index("tok")
    rows, cols = part.shape
    done = []
    for flip in range(2):
        half = part[:, flip * (cols // 2):(flip + 1) * (cols // 2)]
        half = half.reshape((2,) * count + (rows // size, cols // 2))
        left = list(range(count - 1, -1, -1))
        for bit in [0] + list(range(1, count))[:: -1 if flip else 1]:
            axis = left.index(bit)
            mine = (me >> bit) & 1
            keep = lax.dynamic_index_in_dim(half, mine, axis, keepdims=False)
            send = lax.dynamic_index_in_dim(half, 1 - mine, axis, keepdims=False)
            half = keep + swap(send, 1 << bit)
            left.remove(bit)
        done.append(half.astype(jnp.bfloat16))
    return jnp.concatenate(done, axis=1)


def line_gather(x):
    n = lax.axis_size("col")
    z = lax.axis_index("col")
    rows, w = x.shape
    ups, downs = [x], [x]
    for s in range(1, n):
        ups.append(lax.ppermute(ups[-1], "col", [(i, i + 1) for i in range(s - 1, n - 1)]))
        downs.append(lax.ppermute(downs[-1], "col", [(i, i - 1) for i in range(1, n - s + 1)]))
    out = lax.dynamic_update_slice_in_dim(jnp.zeros((rows, n * w), x.dtype), x, z * w, 1)
    for s in range(1, n):
        block = jnp.where(z >= s, ups[s], downs[n - s])
        out = lax.dynamic_update_slice_in_dim(out, block, ((z + n - s) % n) * w, 1)
    return out


def chunks(width):
    if width % (LANES * sum(SHARES)):
        return [(0, width)]
    unit, at, out = width // sum(SHARES), 0, []
    for share in SHARES:
        out.append((at, share * unit))
        at += share * unit
    return out


def body(acts_a, acts_b, whiten_a, whiten_b):
    n, m = lax.axis_size("col"), lax.axis_size("tok")
    tokens, width = acts_a.shape

    parts = chunks(width)
    gathered = [lax.all_gather(acts_a[:, at:at + w], "col", axis=1, tiled=True) for at, w in parts]
    covs, right = [], acts_b
    for g in gathered:
        cov = sum_tokens(dot_tn(g, right))
        cov, right = lax.optimization_barrier((cov, right))
        covs.append(cov)
    covs = [line_gather(c) for c in covs]
    whiten_b, _ = lax.optimization_barrier((whiten_b, cov))
    halves = [jnp.dot(c, whiten_b, preferred_element_type=jnp.float32).astype(jnp.bfloat16) for c in covs]
    halves = [lax.all_gather(h, "col", axis=1, tiled=True) for h in halves]

    total = None
    for (at, w), half in zip(parts, halves):
        half = lax.all_to_all(half, "tok", split_axis=1, concat_axis=0, tiled=True)
        weights = whiten_a.reshape(n, width, -1)[:, at:at + w].reshape(n * w, -1)
        term = dot_tn(weights, half)
        total = term if total is None else total + term
    scale = 1.0 / jnp.sqrt(jnp.float32(tokens * m))
    return total * scale


PIECES = 8
EARLY = 4
PARTS = 4


def schedule(K):
    form = [k + 4 * (k >= EARLY) for k in range(K)]
    join = [f + 1 for f in form]
    whiten = [f + (4 if k < EARLY else 2) for k, f in enumerate(form)]
    return {
        "form": form,
        "join": join[:EARLY],
        "join_late": [None] * EARLY + join[EARLY:],
        "lift": [f + 3 for f in form[:EARLY]],
        "whiten": whiten,
        "spread": [w + 1 for w in whiten],
        "gain": [w + 3 for w in whiten],
    }


def eligible(mesh, acts_a, acts_b):
    n, m = mesh.shape["col"], mesh.shape["tok"]
    width, depth = acts_a.shape[1] // n, acts_b.shape[1] // n
    rows = acts_a.shape[0] // m
    fits = rows % (LANES * PIECES) == 0 and width % LANES == 0 and depth % (2 * LANES) == 0
    return n == 4 and m == 2 * n and fits and width // LANES >= EARLY + 2


def remote(src, dst, send, recv, z, t):
    return pltpu.make_async_remote_copy(
        src_ref=src, dst_ref=dst, send_sem=send, recv_sem=recv,
        device_id={"tok": t, "col": z}, device_id_type=pl.DeviceIdType.MESH)


def kernel(a_hbm, b_hbm, wa_hbm, wb_hbm, out, raw, at, bl, own, xs, xr, rs, rr, keep, cs, cr, wb, wat, stage, hb, hc,
           raw_sem, b_sem, up_sem, bin_sem, wb_sem, ws_sem, wr_sem, st_sem, as_sem, ar_sem, xs_sem, xr_sem, rs_sem, rr_sem, cs_sem, cr_sem,
           hs_sem, hr_sem, ts_sem, tr_sem):
    K, n, _, T = at.shape
    V = bl.shape[2]
    W = wa_hbm.shape[1]
    H = V // 2
    half = LANES // 2
    t, z = lax.axis_index("tok"), lax.axis_index("col")
    g, c = t // 2, t % 2
    sib = t + 1 - 2 * c
    inner = (z == 1) | (z == 2)
    outer = jnp.logical_not(inner)
    edge = z // 2 * 3
    mate = 3 - z
    far = 3 - edge
    hub = 1 + z // 3
    flips = range(1, n)

    def flip(x, d):
        lo, hi = x % 2, x // 2
        return (lo + d % 2) % 2 + 2 * ((hi + d // 2) % 2)

    def flip8(x, d):
        return (x % 2 + d % 2) % 2 + 2 * flip(x // 2, d // 2)

    def load_raw(j):
        return pltpu.make_async_copy(a_hbm.at[:, pl.ds(pl.multiple_of(j * LANES, LANES), LANES)], raw.at[j % 2], raw_sem.at[j % 2])

    def load_stage(q):
        rows = q % n * W + q // n * LANES
        return pltpu.make_async_copy(wa_hbm.at[pl.ds(pl.multiple_of(rows, LANES), LANES), :], stage.at[q % 2], st_sem.at[q % 2])

    own_b = pltpu.make_async_copy(b_hbm, bl.at[0], b_sem)
    load_wb = pltpu.make_async_copy(wb_hbm, wb.at[0], wb_sem)

    def up_b(k):
        rows = pl.ds(k * (T // PIECES), T // PIECES)
        return remote(b_hbm.at[rows, :], bl.at[1, rows, :], up_sem.at[k], bin_sem.at[k], hub, t)

    def post_b(lo, hi):
        for k in range(lo, hi):
            up_b(k).start()

    def post_later(j, jobs):
        for at_j, work in jobs:
            pl.when(j == at_j)(work)

    def share(e, p):
        rows = n * V // (2 * n * PARTS)
        return pl.ds(pl.multiple_of((e * PARTS + p) * rows, rows), rows)

    def up_w(p):
        return remote(wb_hbm.at[share(t, p), :], wb.at[1, share(t, p), :], ws_sem.at[p, 0], wr_sem.at[t, p], hub, t)

    def move_w(e, p, slot, to):
        return remote(wb.at[1, share(e, p), :], wb.at[1, share(e, p), :], ws_sem.at[p, slot], wr_sem.at[e, p], z, to)

    def cousin(d):
        return 2 * flip(g, d) + c

    def move_a(j, src, slot, to):
        return remote(at.at[j, src], at.at[j, src], as_sem.at[slot, j], ar_sem.at[src, j], to, t)

    def swap_x(j, q):
        return remote(xs.at[q], xr.at[j % 2, q], xs_sem.at[q], xr_sem.at[j % 2, q], z, sib)

    def send_r(j, q, d):
        s = flip(g, d)
        return remote(rs.at[j % 2, q, s], rr.at[j % 4, q, d - 1], rs_sem.at[j % 2, q, d - 1], rr_sem.at[j, q, d - 1], z, 2 * s + c)

    def give_c(j, q, b, core, slot, to):
        return remote(cs.at[j, q, core], cr.at[j, b, c], cs_sem.at[j, q, slot], cr_sem.at[j, b, c], to, 2 * g + core)

    def send_c(j, q):
        b = edge if q else z
        return [give_c(j, q, b, 1 - c, 0, z)] + [give_c(j, q, b, k, 1 + k, mate) for k in range(2)]

    def rise_c(j):
        return [give_c(j, 0, z, k, 1 + k, hub) for k in range(2)]

    def pass_c(j, b, k, slot, to):
        return remote(cr.at[j, b, k], cr.at[j, b, k], cs_sem.at[j, 2, slot], cr_sem.at[j, b, k], to, t)

    def move_h(j, src, slot, to):
        return remote(hb.at[j, src], hb.at[j, src], hs_sem.at[j, slot], hr_sem.at[j, src], to, t)

    def send_t(j, d):
        peer = flip8(t, d)
        return remote(hb.at[j, peer // 2, peer % 2], hc.at[j, t], ts_sem.at[j, d - 1], tr_sem.at[j, d - 1], z, peer)

    load_raw(0).start()
    own_b.start()
    load_stage(0).start()
    barrier = pltpu.get_barrier_semaphore()

    def greet(to, who):
        pl.semaphore_signal(barrier, inc=1, device_id={"tok": who, "col": to}, device_id_type=pl.DeviceIdType.MESH)

    for d in range(1, 2 * n):
        greet(z, flip8(t, d))

    @pl.when(inner)
    def _():
        for core in range(2):
            greet(mate, 2 * g + core)
            greet(edge, 2 * g + core)
        pl.semaphore_wait(barrier, 2 * n - 1 + 4)

    @pl.when(outer)
    def _():
        for core in range(2):
            greet(hub, 2 * g + core)
        pl.semaphore_wait(barrier, 2 * n - 1 + 2)

    def post_a(j):
        @pl.when(inner & (j < EARLY))
        def _():
            move_a(j, z, 0, mate).start()

            @pl.when(j < 2)
            def _():
                move_a(j, z, 2, edge).start()

        @pl.when(outer & (j < EARLY))
        def _():
            @pl.when(j == 0)
            def _():
                for p in range(PARTS):
                    up_w(p).start()

            move_a(j, z, 0, hub).start()

            @pl.when(j == EARLY - 1)
            def _():
                post_b(0, PIECES - 4)

    def turn_a(j, _):
        @pl.when(j + 1 < K)
        def _():
            load_raw(j + 1).start()

        load_raw(j).wait()
        at[j, z] = raw[j % 2].T

        @pl.when(j > 0)
        def _():
            post_a(j - 1)
        return 0

    with jax.named_scope("turn_a"):
        lax.fori_loop(0, K, turn_a, 0)
        pl.when(inner)(load_wb.start)
        out[...] = jnp.zeros_like(out)
        post_a(K - 1)

    def turn_w(j):
        for s in range(n):
            q = j * n + s

            @pl.when(q + 1 < K * n)
            def _():
                load_stage(q + 1).start()

            load_stage(q).wait()
            wat[j, :, s * LANES:(s + 1) * LANES] = stage[q % 2].T

    def post_own(lo, hi):
        for j in range(lo, min(hi, K)):
            move_a(j, z, 0, mate).start()

    def post_up(lo, hi):
        for j in range(lo, min(hi, K)):
            move_a(j, z, 0, hub).start()

    def pass_up(j):
        move_a(j, edge, 1, mate).wait_recv()
        move_a(j, edge, 1, mate).start()

    def pass_down(j, src, slot):
        move_a(j, src, slot, edge).wait_recv()
        move_a(j, src, slot, edge).start()

    def turn_ws(lo, hi):
        with jax.named_scope("turn_w"):
            lax.fori_loop(min(lo, K), min(hi, K), lambda j, _: turn_w(j) or 0, 0)

    def when_inner(work, *args):
        with jax.named_scope(work.__name__):
            pl.when(inner)(lambda: work(*args))

    def spread_w(p):
        up_w(p).wait_recv()
        move_w(t, p, 4, sib).start()
        for d in flips:
            move_w(t, p, d, cousin(d)).start()

    def relay_w(p):
        for d in flips:
            move_w(cousin(d), p, 0, sib).wait_recv()
            move_w(cousin(d), p, 4 + d, sib).start()

    def take_w():
        load_wb.wait()
        for p in range(PARTS):
            for d in range(n):
                move_w(2 * flip(g, d) + 1 - c, p, 0, sib).wait_recv()

    for j in range(EARLY):
        turn_ws(2 * j, 2 * j + 2)
        if j < PARTS:
            when_inner(spread_w, j)
        when_inner(pass_down, j, mate, 3)
        if j + 2 < EARLY:
            pl.when(inner)(move_a(j + 2, z, 2, edge).start)
    for j in range(2):
        when_inner(pass_up, j)
    own_b.wait()
    tile = min(2 * LANES, H)

    def both(j, work):
        pl.when(inner | (j < EARLY))(lambda: work(0))
        pl.when(inner & (j >= EARLY))(lambda: work(1))

    def form(j):
        with jax.named_scope("wait_a"):
            @pl.when(inner & (j < EARLY))
            def _():
                pass_down(j, far, 4)

            @pl.when(inner & (j >= EARLY))
            def _():
                @pl.when(j + 1 < K)
                def _():
                    pass_up(j + 1)

                @pl.when(j == EARLY)
                def _():
                    for k in range(PIECES):
                        up_b(k).wait_recv()

                move_a(j, mate, 0, edge).wait_recv()
                move_a(j, far, 0, edge).wait_recv()

            @pl.when(outer & (j < EARLY))
            def _():
                for d in flips:
                    move_a(j, flip(z, d), 0, hub).wait_recv()

        def block(q):
            @pl.when(j > q * EARLY)
            def _():
                swap_x(j, q).wait_send()

            for dst, h in ((xs, 1 - c), (own, c)):
                def step(k, _, dst=dst, h=h):
                    cols = pl.ds(pl.multiple_of(h * H + k * tile, tile), tile)
                    part = jnp.dot(at[j].reshape(n * LANES, T), bl[q, :, cols], preferred_element_type=jnp.float32)
                    dst[q, :, :, pl.ds(pl.multiple_of(k * tile, tile), tile)] = part.reshape(n, LANES, tile)
                    return 0

                lax.fori_loop(0, H // tile, step, 0)
                if dst is own:
                    swap_x(j, q).start()

        both(j, block)

    def split(j):
        def block(q):
            with jax.named_scope("wait_x"):
                swap_x(j, q).wait_recv()

            @pl.when(j > q * EARLY + 1)
            def _():
                for d in flips:
                    send_r(j, q, d).wait_send()

            def step(s, _):
                total = own[q, s] + xr[j % 2, q, s]

                @pl.when(s == g)
                def _():
                    keep[j % 2, q] = total

                rs[j % 2, q, s] = total.astype(rs.dtype)
                return 0

            lax.fori_loop(0, n, step, 0)
            for d in flips:
                send_r(j, q, d).start()

        both(j, block)

    def gather_c(j):
        def block(q):
            with jax.named_scope("wait_r"):
                for d in flips:
                    send_r(j, q, d).wait_recv()
            total = keep[j % 2, q]
            for d in flips:
                total = total + rr[j % 4, q, d - 1].astype(jnp.float32)
            cs[j, q] = total.astype(cs.dtype).reshape(2, half, H)

            @pl.when(inner)
            def _():
                cr[j, edge if q else z, c] = cs[j, q, c]
                for move in send_c(j, q):
                    move.start()
                if q == 0:
                    post_later(j, [(1, lambda: post_own(EARLY + 2, K))])

            if q == 0:
                @pl.when(outer)
                def _():
                    for move in rise_c(j):
                        move.start()
                    post_later(j, [(k, lambda k=k: post_b(PIECES - 4 + k, PIECES - 3 + k)) for k in range(4)])
                    post_later(j, [(EARLY - 1, lambda: post_up(EARLY, K))])

        both(j, block)

    def lift(j):
        for k in range(2):
            pass_c(j, edge, k, k, mate).wait_recv()
            pass_c(j, edge, k, k, mate).start()

    def form_h(j):
        def got(b, k):
            pass_c(j, b, k, 0, mate).wait_recv()

        with jax.named_scope("wait_c"):
            @pl.when(j >= EARLY)
            def _():
                got(edge, 1 - c)

            got(z, 1 - c)
            for k in range(2):
                got(mate, k)
                got(far, k)

        with jax.named_scope("take_w"):
            pl.when(j == 0)(take_w)

        for q, b in ((0, z), (1, edge)):
            for h in range(2):
                def step(k, _, q=q, b=b, h=h):
                    cols = pl.ds(pl.multiple_of(h * H + k * tile, tile), tile)
                    total = jnp.zeros((half, tile), jnp.float32)
                    for p in range(2 * n):
                        total += jnp.dot(cr[j, p // 2, p % 2], wb[q, p * H:(p + 1) * H, cols], preferred_element_type=jnp.float32)
                    hb[j, b, h, :, pl.ds(pl.multiple_of(k * tile, tile), tile)] = total.astype(hb.dtype)
                    return 0

                lax.fori_loop(0, H // tile, step, 0)
            move_h(j, b, 2 * q, mate).start()
            move_h(j, b, 2 * q + 1, edge).start()

    def spread_h(j):
        with jax.named_scope("wait_h"):
            @pl.when(inner)
            def _():
                for src, slot in ((mate, 4), (far, 5)):
                    move_h(j, src, slot, edge).wait_recv()
                    move_h(j, src, slot, edge).start()

            @pl.when(outer)
            def _():
                for src in range(n):
                    move_h(j, src, 0, hub).wait_recv()

        for d in range(1, 2 * n):
            send_t(j, d).start()
        hc[j, t] = hb[j, g, c]

    def gain(j):
        with jax.named_scope("wait_t"):
            for d in range(1, 2 * n):
                send_t(j, d).wait_recv()

        def step(k, _):
            cols = pl.ds(pl.multiple_of(k * tile, tile), tile)
            out[:, cols] += jnp.dot(wat[j], hc[j, :, :, cols].reshape(n * LANES, tile), preferred_element_type=jnp.float32)
            return 0

        lax.fori_loop(0, H // tile, step, 0)

    steps = schedule(K)

    def at_step(i, stage, work, only=None):
        chunk, live = 0, False
        for k, when in enumerate(steps[stage]):
            if when is not None:
                chunk = chunk + k * (i == when).astype(jnp.int32)
                live = live | (i == when)
        if only is not None:
            live = live & only
        with jax.named_scope(stage):
            pl.when(live)(lambda: work(chunk))

    def turn(i, _):
        at_step(i, "form", form)
        at_step(i, "form", split)

        @pl.when(inner & (i + 2 < EARLY))
        def _():
            with jax.named_scope("pass_up"):
                pass_up(i + 2)
                pl.when(i + 3 == EARLY)(lambda: post_own(EARLY, EARLY + 2))

        @pl.when(inner & (i == 2))
        def _():
            with jax.named_scope("relay_w"):
                for p in range(PARTS):
                    relay_w(p)

        at_step(i, "lift", lift, inner)
        at_step(i, "join", gather_c)

        @pl.when(inner & (i == EARLY + 3))
        def _():
            with jax.named_scope("pass_up"):
                pass_up(EARLY)

        at_step(i, "join_late", gather_c, inner)
        at_step(i, "spread", spread_h)
        at_step(i, "whiten", form_h, inner)
        at_step(i, "gain", gain)
        return 0

    lax.fori_loop(0, steps["gain"][-1] + 1, turn, 0)

    @pl.when(inner)
    def _():
        for p in range(PARTS):
            for slot in range(1, 4 + n):
                move_w(t, p, slot, sib).wait_send()
        for q in range(2):
            swap_x(K - 1, q).wait_send()
            for j in range(K - 2, K):
                for d in flips:
                    send_r(j, q, d).wait_send()

    @pl.when(outer)
    def _():
        for p in range(PARTS):
            up_w(p).wait_send()
        for k in range(PIECES):
            up_b(k).wait_send()
        swap_x(0, 0).wait_send()
        for j in range(EARLY - 2, EARLY):
            for d in flips:
                send_r(j, 0, d).wait_send()

    def drain(j, _):
        early = j < EARLY

        @pl.when(inner)
        def _():
            move_a(j, z, 0, mate).wait_send()
            move_a(j, edge, 1, mate).wait_send()

            @pl.when(early)
            def _():
                move_a(j, z, 2, edge).wait_send()
                move_a(j, mate, 3, edge).wait_send()
                move_a(j, far, 4, edge).wait_send()
                for k in range(2):
                    pass_c(j, edge, k, k, mate).wait_send()

            for move in send_c(j, 0):
                move.wait_send()

            @pl.when(jnp.logical_not(early))
            def _():
                for move in send_c(j, 1):
                    move.wait_send()

            for slot in range(6):
                move_h(j, z, slot, mate).wait_send()

        @pl.when(outer)
        def _():
            move_a(j, z, 0, hub).wait_send()

            @pl.when(early)
            def _():
                for move in rise_c(j):
                    move.wait_send()

        for d in range(1, 2 * n):
            send_t(j, d).wait_send()
        return 0

    with jax.named_scope("drain"):
        lax.fori_loop(0, K, drain, 0)


def fused(mesh, acts_a, acts_b, whiten_a, whiten_b):
    n, m = lax.axis_size("col"), lax.axis_size("tok")
    T, W = acts_a.shape
    V = acts_b.shape[1]
    K = W // LANES
    H = V // 2
    bf, f32 = jnp.bfloat16, jnp.float32
    half = LANES // 2
    dma = pltpu.SemaphoreType.DMA
    flops = 2 * (n * W * T * 2 * V + K * half * n * V * V + n * W * W * V // 2)
    total = pl.pallas_call(
        kernel,
        out_shape=jax.ShapeDtypeStruct((W, H), f32),
        in_specs=[pl.BlockSpec(memory_space=pl.ANY)] * 4,
        out_specs=pl.BlockSpec(memory_space=pltpu.VMEM),
        scratch_shapes=[
            pltpu.VMEM((2, T, LANES), bf),
            pltpu.VMEM((K, n, LANES, T), bf),
            pltpu.VMEM((2, T, V), bf),
            pltpu.VMEM((2, n, LANES, H), f32),
            pltpu.VMEM((2, n, LANES, H), f32),
            pltpu.VMEM((2, 2, n, LANES, H), f32),
            pltpu.VMEM((2, 2, n, LANES, H), bf),
            pltpu.VMEM((4, 2, n - 1, LANES, H), bf),
            pltpu.VMEM((2, 2, LANES, H), f32),
            pltpu.VMEM((K, 2, 2, half, H), bf),
            pltpu.VMEM((K, n, 2, half, H), bf),
            pltpu.VMEM((2, n * V, V), bf),
            pltpu.VMEM((K, W, n * LANES), bf),
            pltpu.VMEM((2, LANES, W), bf),
            pltpu.VMEM((K, n, 2, half, H), bf),
            pltpu.VMEM((K, m, half, H), bf),
            dma((2,)), dma, dma((PIECES,)), dma((PIECES,)), dma, dma((PARTS, 4 + n)), dma((2 * n, PARTS)), dma((2,)),
            dma((5, K)), dma((n, K)), dma((2,)), dma((2, 2)), dma((2, 2, n - 1)), dma((K, 2, n - 1)), dma((K, 3, 3)), dma((K, n, 2)),
            dma((K, 6)), dma((K, n)), dma((K, m - 1)), dma((K, m - 1)),
        ],
        compiler_params=pltpu.CompilerParams(collective_id=0, has_side_effects=True, vmem_limit_bytes=67_000_000),
        cost_estimate=pl.CostEstimate(flops=flops, bytes_accessed=2 * (T * (W + V) + n * (W * W + V * V)), transcendentals=0),
    )(acts_a, acts_b, whiten_a, whiten_b)
    return total * (1.0 / jnp.sqrt(jnp.float32(T * m)))


def solution(mesh):
    placed = (P("tok", "col"), P("tok", "col"), P(None, "col"), P(None, "col"))

    def whole(acts_a, acts_b, whiten_a, whiten_b):
        form = functools.partial(fused, mesh) if eligible(mesh, acts_a, acts_b) else body
        return jax.shard_map(form, mesh=mesh, in_specs=placed, out_specs=P("col", "tok"), check_vma=False)(
            acts_a, acts_b, whiten_a, whiten_b)

    return whole
```

```python
import functools

import jax
import jax.numpy as jnp
from jax import lax
from jax.experimental import pallas as pl
from jax.experimental.pallas import tpu as pltpu
from jax.sharding import PartitionSpec as P

LANES = 128
SHARES = (5, 2)


def dot_tn(x, y):
    return lax.dot_general(x, y, (((0,), (0,)), ((), ())), preferred_element_type=jnp.float32)


def swap(x, step):
    return lax.ppermute(x, "tok", [(i, i ^ step) for i in range(lax.axis_size("tok"))])


def sum_tokens(part):
    size = lax.axis_size("tok")
    count = size.bit_length() - 1
    me = lax.axis_index("tok")
    rows, cols = part.shape
    done = []
    for flip in range(2):
        half = part[:, flip * (cols // 2):(flip + 1) * (cols // 2)]
        half = half.reshape((2,) * count + (rows // size, cols // 2))
        left = list(range(count - 1, -1, -1))
        for bit in [0] + list(range(1, count))[:: -1 if flip else 1]:
            axis = left.index(bit)
            mine = (me >> bit) & 1
            keep = lax.dynamic_index_in_dim(half, mine, axis, keepdims=False)
            send = lax.dynamic_index_in_dim(half, 1 - mine, axis, keepdims=False)
            half = keep + swap(send, 1 << bit)
            left.remove(bit)
        done.append(half.astype(jnp.bfloat16))
    return jnp.concatenate(done, axis=1)


def line_gather(x):
    n = lax.axis_size("col")
    z = lax.axis_index("col")
    rows, w = x.shape
    ups, downs = [x], [x]
    for s in range(1, n):
        ups.append(lax.ppermute(ups[-1], "col", [(i, i + 1) for i in range(s - 1, n - 1)]))
        downs.append(lax.ppermute(downs[-1], "col", [(i, i - 1) for i in range(1, n - s + 1)]))
    out = lax.dynamic_update_slice_in_dim(jnp.zeros((rows, n * w), x.dtype), x, z * w, 1)
    for s in range(1, n):
        block = jnp.where(z >= s, ups[s], downs[n - s])
        out = lax.dynamic_update_slice_in_dim(out, block, ((z + n - s) % n) * w, 1)
    return out


def chunks(width):
    if width % (LANES * sum(SHARES)):
        return [(0, width)]
    unit, at, out = width // sum(SHARES), 0, []
    for share in SHARES:
        out.append((at, share * unit))
        at += share * unit
    return out


def body(acts_a, acts_b, whiten_a, whiten_b):
    n, m = lax.axis_size("col"), lax.axis_size("tok")
    tokens, width = acts_a.shape

    parts = chunks(width)
    gathered = [lax.all_gather(acts_a[:, at:at + w], "col", axis=1, tiled=True) for at, w in parts]
    covs, right = [], acts_b
    for g in gathered:
        cov = sum_tokens(dot_tn(g, right))
        cov, right = lax.optimization_barrier((cov, right))
        covs.append(cov)
    covs = [line_gather(c) for c in covs]
    whiten_b, _ = lax.optimization_barrier((whiten_b, cov))
    halves = [jnp.dot(c, whiten_b, preferred_element_type=jnp.float32).astype(jnp.bfloat16) for c in covs]
    halves = [lax.all_gather(h, "col", axis=1, tiled=True) for h in halves]

    total = None
    for (at, w), half in zip(parts, halves):
        half = lax.all_to_all(half, "tok", split_axis=1, concat_axis=0, tiled=True)
        weights = whiten_a.reshape(n, width, -1)[:, at:at + w].reshape(n * w, -1)
        term = dot_tn(weights, half)
        total = term if total is None else total + term
    scale = 1.0 / jnp.sqrt(jnp.float32(tokens * m))
    return total * scale


PIECES = 8
EARLY = 6
PARTS = 4


def schedule(K):
    late = K - EARLY
    form = list(range(EARLY)) + [2 * EARLY + 2 + k for k in range(late)]
    whiten = [EARLY + 2 + k for k in range(EARLY)] + [f + 2 for f in form[EARLY:]]
    return {
        "form": form,
        "join": [EARLY + k for k in range(EARLY)] + [f + 1 for f in form[EARLY:]],
        "join_end": form[:EARLY],
        "lift": [EARLY + k + (k > 0) for k in range(EARLY)],
        "whiten": whiten,
        "spread": [w + 1 for w in whiten],
        "gain": [w + 3 for w in whiten],
    }


def eligible(mesh, acts_a, acts_b):
    n, m = mesh.shape["col"], mesh.shape["tok"]
    width, depth = acts_a.shape[1] // n, acts_b.shape[1] // n
    rows = acts_a.shape[0] // m
    fits = rows % (LANES * PIECES) == 0 and width % LANES == 0 and depth % (2 * LANES) == 0
    return n == 4 and m == 2 * n and fits and width // LANES > EARLY


def remote(src, dst, send, recv, z, t):
    return pltpu.make_async_remote_copy(
        src_ref=src, dst_ref=dst, send_sem=send, recv_sem=recv,
        device_id={"tok": t, "col": z}, device_id_type=pl.DeviceIdType.MESH)


def kernel(a_hbm, b_hbm, wa_hbm, wb_hbm, out, raw, at, bl, own, xs, xr, rs, rr, keep, cs, cr, wb, wat, stage, hb, hc,
           raw_sem, b_sem, up_sem, bin_sem, wb_sem, ws_sem, wr_sem, st_sem, as_sem, ar_sem, xs_sem, xr_sem, rs_sem, rr_sem, cs_sem, cr_sem,
           hs_sem, hr_sem, ts_sem, tr_sem):
    K, n, _, T = at.shape
    V = bl.shape[2]
    W = wa_hbm.shape[1]
    H = V // 2
    half = LANES // 2
    t, z = lax.axis_index("tok"), lax.axis_index("col")
    g, c = t // 2, t % 2
    sib = t + 1 - 2 * c
    inner = (z == 1) | (z == 2)
    outer = jnp.logical_not(inner)
    edge = z // 2 * 3
    mate = 3 - z
    far = 3 - edge
    hub = 1 + z // 3
    flips = range(1, n)

    def flip(x, d):
        lo, hi = x % 2, x // 2
        return (lo + d % 2) % 2 + 2 * ((hi + d // 2) % 2)

    def flip8(x, d):
        return (x % 2 + d % 2) % 2 + 2 * flip(x // 2, d // 2)

    def load_raw(j):
        return pltpu.make_async_copy(a_hbm.at[:, pl.ds(pl.multiple_of(j * LANES, LANES), LANES)], raw.at[j % 2], raw_sem.at[j % 2])

    def load_stage(q):
        rows = q % n * W + q // n * LANES
        return pltpu.make_async_copy(wa_hbm.at[pl.ds(pl.multiple_of(rows, LANES), LANES), :], stage.at[q % 2], st_sem.at[q % 2])

    own_b = pltpu.make_async_copy(b_hbm, bl.at[0], b_sem)
    load_wb = pltpu.make_async_copy(wb_hbm, wb.at[0], wb_sem)

    def up_b(k):
        rows = pl.ds(k * (T // PIECES), T // PIECES)
        return remote(b_hbm.at[rows, :], bl.at[1, rows, :], up_sem.at[k], bin_sem.at[k], hub, t)

    def post_b(lo, hi):
        for k in range(lo, hi):
            up_b(k).start()

    def post_later(j, jobs):
        for at_j, work in jobs:
            pl.when(j == at_j)(work)

    def share(e, p):
        rows = n * V // (2 * n * PARTS)
        return pl.ds(pl.multiple_of((e * PARTS + p) * rows, rows), rows)

    def up_w(p):
        return remote(wb_hbm.at[share(t, p), :], wb.at[1, share(t, p), :], ws_sem.at[p, 0], wr_sem.at[t, p], hub, t)

    def move_w(e, p, slot, to):
        return remote(wb.at[1, share(e, p), :], wb.at[1, share(e, p), :], ws_sem.at[p, slot], wr_sem.at[e, p], z, to)

    def cousin(d):
        return 2 * flip(g, d) + c

    def move_a(j, src, slot, to):
        return remote(at.at[j, src], at.at[j, src], as_sem.at[slot, j], ar_sem.at[src, j], to, t)

    def slot(j, q):
        early = (j < EARLY).astype(jnp.int32)
        return early * j + (1 - early) * (2 * (j - EARLY) + q)

    def swap_x(j, q):
        return remote(xs.at[q], xr.at[j % 2, q], xs_sem.at[q], xr_sem.at[j % 2, q], z, sib)

    def send_r(u, d):
        s = flip(g, d)
        return remote(rs.at[u, s], rr.at[u, d - 1], rs_sem.at[u, d - 1], rr_sem.at[u, d - 1], z, 2 * s + c)

    def give_c(j, q, b, core, slot, to):
        return remote(cs.at[j, q, core], cr.at[j, b, c], cs_sem.at[j, q, slot], cr_sem.at[j, b, c], to, 2 * g + core)

    def send_c(j, q):
        b = edge if q else z
        return [give_c(j, q, b, 1 - c, 0, z)] + [give_c(j, q, b, k, 1 + k, mate) for k in range(2)]

    def rise_c(j):
        return [give_c(j, 0, z, k, 1 + k, hub) for k in range(2)]

    def pass_c(j, b, k, slot, to):
        return remote(cr.at[j, b, k], cr.at[j, b, k], cs_sem.at[j, 2, slot], cr_sem.at[j, b, k], to, t)

    def move_h(j, src, slot, to):
        return remote(hb.at[j, src], hb.at[j, src], hs_sem.at[j, slot], hr_sem.at[j, src], to, t)

    def send_t(j, d):
        peer = flip8(t, d)
        return remote(hb.at[j, peer // 2, peer % 2], hc.at[j, t], ts_sem.at[j, d - 1], tr_sem.at[j, d - 1], z, peer)

    load_raw(0).start()
    own_b.start()
    load_stage(0).start()
    barrier = pltpu.get_barrier_semaphore()

    def greet(to, who):
        pl.semaphore_signal(barrier, inc=1, device_id={"tok": who, "col": to}, device_id_type=pl.DeviceIdType.MESH)

    for d in range(1, 2 * n):
        greet(z, flip8(t, d))

    @pl.when(inner)
    def _():
        for core in range(2):
            greet(mate, 2 * g + core)
            greet(edge, 2 * g + core)
        pl.semaphore_wait(barrier, 2 * n - 1 + 4)

    @pl.when(outer)
    def _():
        for core in range(2):
            greet(hub, 2 * g + core)
        pl.semaphore_wait(barrier, 2 * n - 1 + 2)

    def post_a(j):
        @pl.when(inner & (j < EARLY))
        def _():
            move_a(j, z, 0, mate).start()

            @pl.when(j < 2)
            def _():
                move_a(j, z, 2, edge).start()

        @pl.when(outer & (j < EARLY))
        def _():
            @pl.when(j == 0)
            def _():
                for p in range(PARTS):
                    up_w(p).start()

            move_a(j, z, 0, hub).start()

            @pl.when(j == EARLY - 1)
            def _():
                post_b(0, 2)

    def turn_a(j, _):
        @pl.when(j + 1 < K)
        def _():
            load_raw(j + 1).start()

        load_raw(j).wait()
        at[j, z] = raw[j % 2].T

        @pl.when(j > 0)
        def _():
            post_a(j - 1)
        return 0

    with jax.named_scope("turn_a"):
        lax.fori_loop(0, K, turn_a, 0)
        pl.when(inner)(load_wb.start)
        out[...] = jnp.zeros_like(out)
        post_a(K - 1)

    def turn_w(j):
        for s in range(n):
            q = j * n + s

            @pl.when(q + 1 < K * n)
            def _():
                load_stage(q + 1).start()

            load_stage(q).wait()
            wat[j, :, s * LANES:(s + 1) * LANES] = stage[q % 2].T

    def post_own(lo, hi):
        for j in range(lo, min(hi, K)):
            move_a(j, z, 0, mate).start()

    def post_up(lo, hi):
        for j in range(lo, min(hi, K)):
            move_a(j, z, 0, hub).start()

    def pass_up(j):
        move_a(j, edge, 1, mate).wait_recv()
        move_a(j, edge, 1, mate).start()

    def pass_down(j, src, slot):
        move_a(j, src, slot, edge).wait_recv()
        move_a(j, src, slot, edge).start()

    def turn_ws(lo, hi):
        with jax.named_scope("turn_w"):
            lax.fori_loop(min(lo, K), min(hi, K), lambda j, _: turn_w(j) or 0, 0)

    def when_inner(work, *args):
        with jax.named_scope(work.__name__):
            pl.when(inner)(lambda: work(*args))

    def spread_w(p):
        up_w(p).wait_recv()
        move_w(t, p, 4, sib).start()
        for d in flips:
            move_w(t, p, d, cousin(d)).start()

    def relay_w(p):
        for d in flips:
            move_w(cousin(d), p, 0, sib).wait_recv()
            move_w(cousin(d), p, 4 + d, sib).start()

    def take_w():
        load_wb.wait()
        for p in range(PARTS):
            for d in range(n):
                move_w(2 * flip(g, d) + 1 - c, p, 0, sib).wait_recv()

    for j in range(EARLY):
        turn_ws(2 * j, 2 * j + 2)
        if j < PARTS:
            when_inner(spread_w, j)
        if j < 3:
            when_inner(pass_down, j, mate, 3)
        if j < 2:
            pl.when(inner)(move_a(j + 2, z, 2, edge).start)
    for j in range(2):
        when_inner(pass_up, j)
    own_b.wait()
    tile = min(2 * LANES, H)

    def both(j, work):
        pl.when(inner | (j < EARLY))(lambda: work(0))
        pl.when(inner & (j >= EARLY))(lambda: work(1))

    def form(j):
        with jax.named_scope("wait_a"):
            @pl.when(inner & (j < EARLY))
            def _():
                pass_down(j, far, 4)
                post_later(j, [(0, lambda: pass_down(3, mate, 3))])
                for k in range(4, EARLY):
                    post_later(j, [(k - 2, lambda k=k: (move_a(k, z, 2, edge).start(), pass_down(k, mate, 3)) and None)])

            @pl.when(inner & (j >= EARLY))
            def _():
                @pl.when(j + 1 < K)
                def _():
                    pass_up(j + 1)

                @pl.when(j == EARLY)
                def _():
                    for k in range(PIECES):
                        up_b(k).wait_recv()

                move_a(j, mate, 0, edge).wait_recv()
                move_a(j, far, 0, edge).wait_recv()

            @pl.when(outer & (j < EARLY))
            def _():
                for d in flips:
                    move_a(j, flip(z, d), 0, hub).wait_recv()

        def block(q):
            @pl.when(j > q * EARLY)
            def _():
                swap_x(j, q).wait_send()

            for dst, h in ((xs, 1 - c), (own, c)):
                def step(k, _, dst=dst, h=h):
                    cols = pl.ds(pl.multiple_of(h * H + k * tile, tile), tile)
                    part = jnp.dot(at[j].reshape(n * LANES, T), bl[q, :, cols], preferred_element_type=jnp.float32)
                    dst[q, :, :, pl.ds(pl.multiple_of(k * tile, tile), tile)] = part.reshape(n, LANES, tile)
                    return 0

                lax.fori_loop(0, H // tile, step, 0)
                if dst is own:
                    swap_x(j, q).start()

        both(j, block)

    def split(j):
        def block(q):
            with jax.named_scope("wait_x"):
                swap_x(j, q).wait_recv()

            u = slot(j, q)

            @pl.when((j >= EARLY) & (u < EARLY))
            def _():
                for d in flips:
                    send_r(u, d).wait_send()

            def step(s, _):
                total = own[q, s] + xr[j % 2, q, s]

                @pl.when(s == g)
                def _():
                    keep[u] = total

                rs[u, s] = total.astype(rs.dtype)
                return 0

            lax.fori_loop(0, n, step, 0)
            for d in flips:
                send_r(u, d).start()

        both(j, block)

    def gather_c(j):
        def block(q):
            with jax.named_scope("wait_r"):
                u = slot(j, q)
                for d in flips:
                    send_r(u, d).wait_recv()
            total = keep[u]
            for d in flips:
                total = total + rr[u, d - 1].astype(jnp.float32)
            cs[j, q] = total.astype(cs.dtype).reshape(2, half, H)

            @pl.when(inner)
            def _():
                cr[j, edge if q else z, c] = cs[j, q, c]
                for move in send_c(j, q):
                    move.start()

            if q == 0:
                @pl.when(outer)
                def _():
                    for move in rise_c(j):
                        move.start()
                    ends = [2, 4] + [min(4 + k, PIECES) for k in range(1, EARLY - 1)] + [PIECES]
                    post_later(j, [(k, lambda k=k: post_b(ends[k], ends[k + 1])) for k in range(EARLY)])
                    post_later(j, [(EARLY - 1, lambda: post_up(EARLY, K))])

        both(j, block)

    def lift(j):
        for k in range(2):
            pass_c(j, edge, k, k, mate).wait_recv()
            pass_c(j, edge, k, k, mate).start()

    def form_h(j):
        def got(b, k):
            pass_c(j, b, k, 0, mate).wait_recv()

        with jax.named_scope("wait_c"):
            @pl.when(j >= EARLY)
            def _():
                got(edge, 1 - c)

            got(z, 1 - c)
            for k in range(2):
                got(mate, k)
                got(far, k)

        with jax.named_scope("take_w"):
            pl.when(j == 0)(take_w)

        for q, b in ((0, z), (1, edge)):
            for h in range(2):
                def step(k, _, q=q, b=b, h=h):
                    cols = pl.ds(pl.multiple_of(h * H + k * tile, tile), tile)
                    total = jnp.zeros((half, tile), jnp.float32)
                    for p in range(2 * n):
                        total += jnp.dot(cr[j, p // 2, p % 2], wb[q, p * H:(p + 1) * H, cols], preferred_element_type=jnp.float32)
                    hb[j, b, h, :, pl.ds(pl.multiple_of(k * tile, tile), tile)] = total.astype(hb.dtype)
                    return 0

                lax.fori_loop(0, H // tile, step, 0)
            move_h(j, b, 2 * q, mate).start()
            move_h(j, b, 2 * q + 1, edge).start()
        post_later(j, [(0, lambda: post_own(EARLY, EARLY + 1)), (1, lambda: post_own(EARLY + 1, K))])

    def spread_h(j):
        with jax.named_scope("wait_h"):
            @pl.when(inner)
            def _():
                for src, slot in ((mate, 4), (far, 5)):
                    move_h(j, src, slot, edge).wait_recv()
                    move_h(j, src, slot, edge).start()

            @pl.when(outer)
            def _():
                for src in range(n):
                    move_h(j, src, 0, hub).wait_recv()

        for d in range(1, 2 * n):
            send_t(j, d).start()
        hc[j, t] = hb[j, g, c]

    def gain(j):
        with jax.named_scope("wait_t"):
            for d in range(1, 2 * n):
                send_t(j, d).wait_recv()

        def step(k, _):
            cols = pl.ds(pl.multiple_of(k * tile, tile), tile)
            out[:, cols] += jnp.dot(wat[j], hc[j, :, :, cols].reshape(n * LANES, tile), preferred_element_type=jnp.float32)
            return 0

        lax.fori_loop(0, H // tile, step, 0)

    steps = schedule(K)

    def at_step(i, stage, work, only=None):
        chunk, live = 0, False
        for k, when in enumerate(steps[stage]):
            if when is not None:
                chunk = chunk + k * (i == when).astype(jnp.int32)
                live = live | (i == when)
        if only is not None:
            live = live & only
        with jax.named_scope(stage):
            pl.when(live)(lambda: work(chunk))

    def turn(i, _):
        at_step(i, "form", form)
        at_step(i, "form", split)

        @pl.when(inner & (i + 2 < EARLY))
        def _():
            with jax.named_scope("pass_up"):
                pass_up(i + 2)

        @pl.when(inner & (i == EARLY - 1))
        def _():
            with jax.named_scope("relay_w"):
                for p in range(PARTS):
                    relay_w(p)

        at_step(i, "join", gather_c, inner)
        at_step(i, "join_end", gather_c, outer)

        @pl.when(inner & (i == 2 * EARLY + 1))
        def _():
            with jax.named_scope("pass_up"):
                pass_up(EARLY)

        at_step(i, "lift", lift, inner)
        at_step(i, "whiten", form_h, inner)
        at_step(i, "spread", spread_h)
        at_step(i, "gain", gain)
        return 0

    lax.fori_loop(0, steps["gain"][-1] + 1, turn, 0)

    @pl.when(inner)
    def _():
        for p in range(PARTS):
            for slot in range(1, 4 + n):
                move_w(t, p, slot, sib).wait_send()
        for q in range(2):
            swap_x(K - 1, q).wait_send()
        for u in range(max(EARLY, 2 * (K - EARLY))):
            for d in flips:
                send_r(u, d).wait_send()

    @pl.when(outer)
    def _():
        for p in range(PARTS):
            up_w(p).wait_send()
        for k in range(PIECES):
            up_b(k).wait_send()
        swap_x(0, 0).wait_send()
        for u in range(EARLY):
            for d in flips:
                send_r(u, d).wait_send()

    def drain(j, _):
        early = j < EARLY

        @pl.when(inner)
        def _():
            move_a(j, z, 0, mate).wait_send()
            move_a(j, edge, 1, mate).wait_send()

            @pl.when(early)
            def _():
                move_a(j, z, 2, edge).wait_send()
                move_a(j, mate, 3, edge).wait_send()
                move_a(j, far, 4, edge).wait_send()
                for k in range(2):
                    pass_c(j, edge, k, k, mate).wait_send()

            for move in send_c(j, 0):
                move.wait_send()

            @pl.when(jnp.logical_not(early))
            def _():
                for move in send_c(j, 1):
                    move.wait_send()

            for slot in range(6):
                move_h(j, z, slot, mate).wait_send()

        @pl.when(outer)
        def _():
            move_a(j, z, 0, hub).wait_send()

            @pl.when(early)
            def _():
                for move in rise_c(j):
                    move.wait_send()

        for d in range(1, 2 * n):
            send_t(j, d).wait_send()
        return 0

    with jax.named_scope("drain"):
        lax.fori_loop(0, K, drain, 0)


def fused(mesh, acts_a, acts_b, whiten_a, whiten_b):
    n, m = lax.axis_size("col"), lax.axis_size("tok")
    T, W = acts_a.shape
    V = acts_b.shape[1]
    K = W // LANES
    H = V // 2
    bf, f32 = jnp.bfloat16, jnp.float32
    half = LANES // 2
    units = max(EARLY, 2 * (K - EARLY))
    dma = pltpu.SemaphoreType.DMA
    flops = 2 * (n * W * T * 2 * V + K * half * n * V * V + n * W * W * V // 2)
    total = pl.pallas_call(
        kernel,
        out_shape=jax.ShapeDtypeStruct((W, H), f32),
        in_specs=[pl.BlockSpec(memory_space=pl.ANY)] * 4,
        out_specs=pl.BlockSpec(memory_space=pltpu.VMEM),
        scratch_shapes=[
            pltpu.VMEM((2, T, LANES), bf),
            pltpu.VMEM((K, n, LANES, T), bf),
            pltpu.VMEM((2, T, V), bf),
            pltpu.VMEM((2, n, LANES, H), f32),
            pltpu.VMEM((2, n, LANES, H), f32),
            pltpu.VMEM((2, 2, n, LANES, H), f32),
            pltpu.VMEM((units, n, LANES, H), bf),
            pltpu.VMEM((units, n - 1, LANES, H), bf),
            pltpu.VMEM((units, LANES, H), f32),
            pltpu.VMEM((K, 2, 2, half, H), bf),
            pltpu.VMEM((K, n, 2, half, H), bf),
            pltpu.VMEM((2, n * V, V), bf),
            pltpu.VMEM((K, W, n * LANES), bf),
            pltpu.VMEM((2, LANES, W), bf),
            pltpu.VMEM((K, n, 2, half, H), bf),
            pltpu.VMEM((K, m, half, H), bf),
            dma((2,)), dma, dma((PIECES,)), dma((PIECES,)), dma, dma((PARTS, 4 + n)), dma((2 * n, PARTS)), dma((2,)),
            dma((5, K)), dma((n, K)), dma((2,)), dma((2, 2)), dma((units, n - 1)), dma((units, n - 1)), dma((K, 3, 3)), dma((K, n, 2)),
            dma((K, 6)), dma((K, n)), dma((K, m - 1)), dma((K, m - 1)),
        ],
        compiler_params=pltpu.CompilerParams(collective_id=0, has_side_effects=True, vmem_limit_bytes=67_000_000),
        cost_estimate=pl.CostEstimate(flops=flops, bytes_accessed=2 * (T * (W + V) + n * (W * W + V * V)), transcendentals=0),
    )(acts_a, acts_b, whiten_a, whiten_b)
    return total * (1.0 / jnp.sqrt(jnp.float32(T * m)))


def solution(mesh):
    placed = (P("tok", "col"), P("tok", "col"), P(None, "col"), P(None, "col"))

    def whole(acts_a, acts_b, whiten_a, whiten_b):
        form = functools.partial(fused, mesh) if eligible(mesh, acts_a, acts_b) else body
        return jax.shard_map(form, mesh=mesh, in_specs=placed, out_specs=P("col", "tok"), check_vma=False)(
            acts_a, acts_b, whiten_a, whiten_b)

    return whole
```

```python
import functools

import jax
import jax.numpy as jnp
from jax import lax
from jax.experimental import pallas as pl
from jax.experimental.pallas import tpu as pltpu
from jax.sharding import PartitionSpec as P

LANES = 128
SHARES = (5, 2)


def dot_tn(x, y):
    return lax.dot_general(x, y, (((0,), (0,)), ((), ())), preferred_element_type=jnp.float32)


def swap(x, step):
    return lax.ppermute(x, "tok", [(i, i ^ step) for i in range(lax.axis_size("tok"))])


def sum_tokens(part):
    size = lax.axis_size("tok")
    count = size.bit_length() - 1
    me = lax.axis_index("tok")
    rows, cols = part.shape
    done = []
    for flip in range(2):
        half = part[:, flip * (cols // 2):(flip + 1) * (cols // 2)]
        half = half.reshape((2,) * count + (rows // size, cols // 2))
        left = list(range(count - 1, -1, -1))
        for bit in [0] + list(range(1, count))[:: -1 if flip else 1]:
            axis = left.index(bit)
            mine = (me >> bit) & 1
            keep = lax.dynamic_index_in_dim(half, mine, axis, keepdims=False)
            send = lax.dynamic_index_in_dim(half, 1 - mine, axis, keepdims=False)
            half = keep + swap(send, 1 << bit)
            left.remove(bit)
        done.append(half.astype(jnp.bfloat16))
    return jnp.concatenate(done, axis=1)


def line_gather(x):
    n = lax.axis_size("col")
    z = lax.axis_index("col")
    rows, w = x.shape
    ups, downs = [x], [x]
    for s in range(1, n):
        ups.append(lax.ppermute(ups[-1], "col", [(i, i + 1) for i in range(s - 1, n - 1)]))
        downs.append(lax.ppermute(downs[-1], "col", [(i, i - 1) for i in range(1, n - s + 1)]))
    out = lax.dynamic_update_slice_in_dim(jnp.zeros((rows, n * w), x.dtype), x, z * w, 1)
    for s in range(1, n):
        block = jnp.where(z >= s, ups[s], downs[n - s])
        out = lax.dynamic_update_slice_in_dim(out, block, ((z + n - s) % n) * w, 1)
    return out


def chunks(width):
    if width % (LANES * sum(SHARES)):
        return [(0, width)]
    unit, at, out = width // sum(SHARES), 0, []
    for share in SHARES:
        out.append((at, share * unit))
        at += share * unit
    return out


def body(acts_a, acts_b, whiten_a, whiten_b):
    n, m = lax.axis_size("col"), lax.axis_size("tok")
    tokens, width = acts_a.shape

    parts = chunks(width)
    gathered = [lax.all_gather(acts_a[:, at:at + w], "col", axis=1, tiled=True) for at, w in parts]
    covs, right = [], acts_b
    for g in gathered:
        cov = sum_tokens(dot_tn(g, right))
        cov, right = lax.optimization_barrier((cov, right))
        covs.append(cov)
    covs = [line_gather(c) for c in covs]
    whiten_b, _ = lax.optimization_barrier((whiten_b, cov))
    halves = [jnp.dot(c, whiten_b, preferred_element_type=jnp.float32).astype(jnp.bfloat16) for c in covs]
    halves = [lax.all_gather(h, "col", axis=1, tiled=True) for h in halves]

    total = None
    for (at, w), half in zip(parts, halves):
        half = lax.all_to_all(half, "tok", split_axis=1, concat_axis=0, tiled=True)
        weights = whiten_a.reshape(n, width, -1)[:, at:at + w].reshape(n * w, -1)
        term = dot_tn(weights, half)
        total = term if total is None else total + term
    scale = 1.0 / jnp.sqrt(jnp.float32(tokens * m))
    return total * scale


PIECES = 8
EARLY = 6
PARTS = 4


def schedule(K):
    late = K - EARLY
    form = list(range(EARLY)) + [2 * EARLY + 1 + k for k in range(late)]
    whiten = [EARLY + 2 + k for k in range(EARLY)] + [f + 2 for f in form[EARLY:]]
    return {
        "form": form,
        "join": [EARLY + k for k in range(EARLY)] + [f + 1 for f in form[EARLY:]],
        "join_top": [None, None, 3, None, 5, None],
        "join_end": [0, 2, None, 4, None, 5],
        "lift": [EARLY + k for k in range(EARLY)],
        "whiten": whiten,
        "spread": [w + 1 for w in whiten],
        "gain": [w + 3 for w in whiten],
    }


def eligible(mesh, acts_a, acts_b):
    n, m = mesh.shape["col"], mesh.shape["tok"]
    width, depth = acts_a.shape[1] // n, acts_b.shape[1] // n
    rows = acts_a.shape[0] // m
    fits = rows % (LANES * PIECES) == 0 and width % LANES == 0 and depth % (2 * LANES) == 0
    return n == 4 and m == 2 * n and fits and width // LANES > EARLY


def remote(src, dst, send, recv, z, t):
    return pltpu.make_async_remote_copy(
        src_ref=src, dst_ref=dst, send_sem=send, recv_sem=recv,
        device_id={"tok": t, "col": z}, device_id_type=pl.DeviceIdType.MESH)


def kernel(a_hbm, b_hbm, wa_hbm, wb_hbm, out, raw, at, bl, own, xs, xr, rs, rr, keep, cs, cr, wb, wat, stage, hb, hc,
           raw_sem, b_sem, up_sem, bin_sem, wb_sem, ws_sem, wr_sem, st_sem, as_sem, ar_sem, xs_sem, xr_sem, rs_sem, rr_sem, cs_sem, cr_sem,
           hs_sem, hr_sem, ts_sem, tr_sem):
    K, n, _, T = at.shape
    V = bl.shape[2]
    W = wa_hbm.shape[1]
    H = V // 2
    half = LANES // 2
    t, z = lax.axis_index("tok"), lax.axis_index("col")
    g, c = t // 2, t % 2
    sib = t + 1 - 2 * c
    inner = (z == 1) | (z == 2)
    outer = jnp.logical_not(inner)
    edge = z // 2 * 3
    mate = 3 - z
    far = 3 - edge
    hub = 1 + z // 3
    flips = range(1, n)

    def flip(x, d):
        lo, hi = x % 2, x // 2
        return (lo + d % 2) % 2 + 2 * ((hi + d // 2) % 2)

    def flip8(x, d):
        return (x % 2 + d % 2) % 2 + 2 * flip(x // 2, d // 2)

    def load_raw(j):
        return pltpu.make_async_copy(a_hbm.at[:, pl.ds(pl.multiple_of(j * LANES, LANES), LANES)], raw.at[j % 2], raw_sem.at[j % 2])

    def load_stage(q):
        rows = q % n * W + q // n * LANES
        return pltpu.make_async_copy(wa_hbm.at[pl.ds(pl.multiple_of(rows, LANES), LANES), :], stage.at[q % 2], st_sem.at[q % 2])

    own_b = pltpu.make_async_copy(b_hbm, bl.at[0], b_sem)
    load_wb = pltpu.make_async_copy(wb_hbm, wb.at[0], wb_sem)

    def up_b(k):
        rows = pl.ds(k * (T // PIECES), T // PIECES)
        return remote(b_hbm.at[rows, :], bl.at[1, rows, :], up_sem.at[k], bin_sem.at[k], hub, t)

    def post_b(lo, hi):
        for k in range(lo, hi):
            up_b(k).start()

    def post_later(j, jobs):
        for at_j, work in jobs:
            pl.when(j == at_j)(work)

    def share(e, p):
        rows = n * V // (2 * n * PARTS)
        return pl.ds(pl.multiple_of((e * PARTS + p) * rows, rows), rows)

    def up_w(p):
        return remote(wb_hbm.at[share(t, p), :], wb.at[1, share(t, p), :], ws_sem.at[p, 0], wr_sem.at[t, p], hub, t)

    def move_w(e, p, slot, to):
        return remote(wb.at[1, share(e, p), :], wb.at[1, share(e, p), :], ws_sem.at[p, slot], wr_sem.at[e, p], z, to)

    def cousin(d):
        return 2 * flip(g, d) + c

    def move_a(j, src, slot, to):
        return remote(at.at[j, src], at.at[j, src], as_sem.at[slot, j], ar_sem.at[src, j], to, t)

    def slot(j, q):
        early = (j < EARLY).astype(jnp.int32)
        return early * j + (1 - early) * (2 * (j - EARLY) + q)

    def swap_x(j, q):
        return remote(xs.at[q], xr.at[j % 2, q], xs_sem.at[q], xr_sem.at[j % 2, q], z, sib)

    def send_r(u, d):
        s = flip(g, d)
        return remote(rs.at[u, s], rr.at[u, d - 1], rs_sem.at[u, d - 1], rr_sem.at[u, d - 1], z, 2 * s + c)

    def give_c(j, q, b, core, slot, to):
        return remote(cs.at[j, q, core], cr.at[j, b, c], cs_sem.at[j, q, slot], cr_sem.at[j, b, c], to, 2 * g + core)

    def send_c(j, q):
        b = edge if q else z
        return [give_c(j, q, b, 1 - c, 0, z)] + [give_c(j, q, b, k, 1 + k, mate) for k in range(2)]

    def rise_c(j):
        return [give_c(j, 0, z, k, 1 + k, hub) for k in range(2)]

    def pass_c(j, b, k, slot, to):
        return remote(cr.at[j, b, k], cr.at[j, b, k], cs_sem.at[j, 2, slot], cr_sem.at[j, b, k], to, t)

    def move_h(j, src, slot, to):
        return remote(hb.at[j, src], hb.at[j, src], hs_sem.at[j, slot], hr_sem.at[j, src], to, t)

    def send_t(j, d):
        peer = flip8(t, d)
        return remote(hb.at[j, peer // 2, peer % 2], hc.at[j, t], ts_sem.at[j, d - 1], tr_sem.at[j, d - 1], z, peer)

    load_raw(0).start()
    own_b.start()
    load_stage(0).start()
    barrier = pltpu.get_barrier_semaphore()

    def greet(to, who):
        pl.semaphore_signal(barrier, inc=1, device_id={"tok": who, "col": to}, device_id_type=pl.DeviceIdType.MESH)

    for d in range(1, 2 * n):
        greet(z, flip8(t, d))

    @pl.when(inner)
    def _():
        for core in range(2):
            greet(mate, 2 * g + core)
            greet(edge, 2 * g + core)
        pl.semaphore_wait(barrier, 2 * n - 1 + 4)

    @pl.when(outer)
    def _():
        for core in range(2):
            greet(hub, 2 * g + core)
        pl.semaphore_wait(barrier, 2 * n - 1 + 2)

    def post_a(j):
        @pl.when(inner & (j < EARLY))
        def _():
            move_a(j, z, 0, mate).start()

            @pl.when(j < 2)
            def _():
                move_a(j, z, 2, edge).start()

        @pl.when(outer & (j < EARLY))
        def _():
            @pl.when(j == 0)
            def _():
                for p in range(PARTS):
                    up_w(p).start()

            move_a(j, z, 0, hub).start()

            @pl.when(j == EARLY - 1)
            def _():
                post_b(0, 2)

    def turn_a(j, _):
        @pl.when(j + 1 < K)
        def _():
            load_raw(j + 1).start()

        load_raw(j).wait()
        at[j, z] = raw[j % 2].T

        @pl.when(j > 0)
        def _():
            post_a(j - 1)
        return 0

    with jax.named_scope("turn_a"):
        lax.fori_loop(0, K, turn_a, 0)
        pl.when(inner)(load_wb.start)
        out[...] = jnp.zeros_like(out)
        post_a(K - 1)

    def turn_w(j):
        for s in range(n):
            q = j * n + s

            @pl.when(q + 1 < K * n)
            def _():
                load_stage(q + 1).start()

            load_stage(q).wait()
            wat[j, :, s * LANES:(s + 1) * LANES] = stage[q % 2].T

    def post_own(lo, hi):
        for j in range(lo, min(hi, K)):
            move_a(j, z, 0, mate).start()

    def post_up(lo, hi):
        for j in range(lo, min(hi, K)):
            move_a(j, z, 0, hub).start()

    def pass_up(j):
        move_a(j, edge, 1, mate).wait_recv()
        move_a(j, edge, 1, mate).start()

    def pass_down(j, src, slot):
        move_a(j, src, slot, edge).wait_recv()
        move_a(j, src, slot, edge).start()

    def turn_ws(lo, hi):
        with jax.named_scope("turn_w"):
            lax.fori_loop(min(lo, K), min(hi, K), lambda j, _: turn_w(j) or 0, 0)

    def when_inner(work, *args):
        with jax.named_scope(work.__name__):
            pl.when(inner)(lambda: work(*args))

    def spread_w(p):
        up_w(p).wait_recv()
        move_w(t, p, 4, sib).start()
        for d in flips:
            move_w(t, p, d, cousin(d)).start()

    def relay_w(p):
        for d in flips:
            move_w(cousin(d), p, 0, sib).wait_recv()
            move_w(cousin(d), p, 4 + d, sib).start()

    def take_w():
        load_wb.wait()
        for p in range(PARTS):
            for d in range(n):
                move_w(2 * flip(g, d) + 1 - c, p, 0, sib).wait_recv()

    for j in range(EARLY):
        turn_ws(2 * j, 2 * j + 2)
        if j < PARTS:
            when_inner(spread_w, j)
        if j < 3:
            when_inner(pass_down, j, mate, 3)
        if j < 2:
            pl.when(inner)(move_a(j + 2, z, 2, edge).start)
    for j in range(2):
        when_inner(pass_up, j)
    own_b.wait()
    tile = min(2 * LANES, H)

    def both(j, work):
        pl.when(inner | (j < EARLY))(lambda: work(0))
        pl.when(inner & (j >= EARLY))(lambda: work(1))

    def form(j):
        with jax.named_scope("wait_a"):
            @pl.when(inner & (j < EARLY))
            def _():
                pass_down(j, far, 4)
                post_later(j, [(0, lambda: pass_down(3, mate, 3))])
                for k in range(4, EARLY):
                    post_later(j, [(k - 2, lambda k=k: (move_a(k, z, 2, edge).start(), pass_down(k, mate, 3)) and None)])

            @pl.when(inner & (j >= EARLY))
            def _():
                @pl.when(j + 1 < K)
                def _():
                    pass_up(j + 1)

                @pl.when(j == EARLY)
                def _():
                    for k in range(PIECES):
                        up_b(k).wait_recv()

                move_a(j, mate, 0, edge).wait_recv()
                move_a(j, far, 0, edge).wait_recv()

            @pl.when(outer & (j < EARLY))
            def _():
                for d in flips:
                    move_a(j, flip(z, d), 0, hub).wait_recv()

        def block(q):
            @pl.when(j > q * EARLY)
            def _():
                swap_x(j, q).wait_send()

            for dst, h in ((xs, 1 - c), (own, c)):
                def step(k, _, dst=dst, h=h):
                    cols = pl.ds(pl.multiple_of(h * H + k * tile, tile), tile)
                    part = jnp.dot(at[j].reshape(n * LANES, T), bl[q, :, cols], preferred_element_type=jnp.float32)
                    dst[q, :, :, pl.ds(pl.multiple_of(k * tile, tile), tile)] = part.reshape(n, LANES, tile)
                    return 0

                lax.fori_loop(0, H // tile, step, 0)
                if dst is own:
                    swap_x(j, q).start()

        both(j, block)

    def split(j):
        def block(q):
            with jax.named_scope("wait_x"):
                swap_x(j, q).wait_recv()

            u = slot(j, q)

            @pl.when((j >= EARLY) & (u < EARLY))
            def _():
                for d in flips:
                    send_r(u, d).wait_send()

            def step(s, _):
                total = own[q, s] + xr[j % 2, q, s]

                @pl.when(s == g)
                def _():
                    keep[u] = total

                rs[u, s] = total.astype(rs.dtype)
                return 0

            lax.fori_loop(0, n, step, 0)
            for d in flips:
                send_r(u, d).start()

        both(j, block)

    def gather_c(j):
        def block(q):
            with jax.named_scope("wait_r"):
                u = slot(j, q)
                for d in flips:
                    send_r(u, d).wait_recv()
            total = keep[u]
            for d in flips:
                total = total + rr[u, d - 1].astype(jnp.float32)
            cs[j, q] = total.astype(cs.dtype).reshape(2, half, H)

            @pl.when(inner)
            def _():
                cr[j, edge if q else z, c] = cs[j, q, c]
                for move in send_c(j, q):
                    move.start()

            if q == 0:
                @pl.when(outer)
                def _():
                    for move in rise_c(j):
                        move.start()
                    ends = [2, 4] + [min(4 + k, PIECES) for k in range(1, EARLY - 1)] + [PIECES]
                    post_later(j, [(k, lambda k=k: post_b(ends[k], ends[k + 1])) for k in range(EARLY)])
                    post_later(j, [(EARLY - 1, lambda: post_up(EARLY, K))])

        both(j, block)

    def lift(j):
        for k in range(2):
            pass_c(j, edge, k, k, mate).wait_recv()
            pass_c(j, edge, k, k, mate).start()

    def form_h(j):
        def got(b, k):
            pass_c(j, b, k, 0, mate).wait_recv()

        with jax.named_scope("wait_c"):
            @pl.when(j >= EARLY)
            def _():
                got(edge, 1 - c)

            got(z, 1 - c)
            for k in range(2):
                got(mate, k)
                got(far, k)

        with jax.named_scope("take_w"):
            pl.when(j == 0)(take_w)

        for q, b in ((0, z), (1, edge)):
            for h in range(2):
                def step(k, _, q=q, b=b, h=h):
                    cols = pl.ds(pl.multiple_of(h * H + k * tile, tile), tile)
                    total = jnp.zeros((half, tile), jnp.float32)
                    for p in range(2 * n):
                        total += jnp.dot(cr[j, p // 2, p % 2], wb[q, p * H:(p + 1) * H, cols], preferred_element_type=jnp.float32)
                    hb[j, b, h, :, pl.ds(pl.multiple_of(k * tile, tile), tile)] = total.astype(hb.dtype)
                    return 0

                lax.fori_loop(0, H // tile, step, 0)
            move_h(j, b, 2 * q, mate).start()
            move_h(j, b, 2 * q + 1, edge).start()
        post_later(j, [(3, lambda: post_own(EARLY, EARLY + 1)), (4, lambda: post_own(EARLY + 1, K))])

    def spread_h(j):
        with jax.named_scope("wait_h"):
            @pl.when(inner)
            def _():
                for src, slot in ((mate, 4), (far, 5)):
                    move_h(j, src, slot, edge).wait_recv()
                    move_h(j, src, slot, edge).start()

            @pl.when(outer)
            def _():
                for src in range(n):
                    move_h(j, src, 0, hub).wait_recv()

        for d in range(1, 2 * n):
            send_t(j, d).start()
        hc[j, t] = hb[j, g, c]

    def gain(j):
        with jax.named_scope("wait_t"):
            for d in range(1, 2 * n):
                send_t(j, d).wait_recv()

        def step(k, _):
            cols = pl.ds(pl.multiple_of(k * tile, tile), tile)
            out[:, cols] += jnp.dot(wat[j], hc[j, :, :, cols].reshape(n * LANES, tile), preferred_element_type=jnp.float32)
            return 0

        lax.fori_loop(0, H // tile, step, 0)

    steps = schedule(K)

    def at_step(i, stage, work, only=None):
        chunk, live = 0, False
        for k, when in enumerate(steps[stage]):
            if when is not None:
                chunk = chunk + k * (i == when).astype(jnp.int32)
                live = live | (i == when)
        if only is not None:
            live = live & only
        with jax.named_scope(stage):
            pl.when(live)(lambda: work(chunk))

    def turn(i, _):
        at_step(i, "join_top", gather_c, outer)
        at_step(i, "form", form)
        at_step(i, "form", split)

        @pl.when(inner & (i + 2 < EARLY))
        def _():
            with jax.named_scope("pass_up"):
                pass_up(i + 2)

        @pl.when(inner & (i == EARLY - 1))
        def _():
            with jax.named_scope("relay_w"):
                for p in range(PARTS):
                    relay_w(p)

        at_step(i, "join", gather_c, inner)
        at_step(i, "join_end", gather_c, outer)

        @pl.when(inner & (i == 2 * EARLY))
        def _():
            with jax.named_scope("pass_up"):
                pass_up(EARLY)

        at_step(i, "whiten", form_h, inner)
        at_step(i, "spread", spread_h)
        at_step(i, "lift", lift, inner)
        at_step(i, "gain", gain)
        return 0

    lax.fori_loop(0, steps["gain"][-1] + 1, turn, 0)

    @pl.when(inner)
    def _():
        for p in range(PARTS):
            for slot in range(1, 4 + n):
                move_w(t, p, slot, sib).wait_send()
        for q in range(2):
            swap_x(K - 1, q).wait_send()
        for u in range(max(EARLY, 2 * (K - EARLY))):
            for d in flips:
                send_r(u, d).wait_send()

    @pl.when(outer)
    def _():
        for p in range(PARTS):
            up_w(p).wait_send()
        for k in range(PIECES):
            up_b(k).wait_send()
        swap_x(0, 0).wait_send()
        for u in range(EARLY):
            for d in flips:
                send_r(u, d).wait_send()

    def drain(j, _):
        early = j < EARLY

        @pl.when(inner)
        def _():
            move_a(j, z, 0, mate).wait_send()
            move_a(j, edge, 1, mate).wait_send()

            @pl.when(early)
            def _():
                move_a(j, z, 2, edge).wait_send()
                move_a(j, mate, 3, edge).wait_send()
                move_a(j, far, 4, edge).wait_send()
                for k in range(2):
                    pass_c(j, edge, k, k, mate).wait_send()

            for move in send_c(j, 0):
                move.wait_send()

            @pl.when(jnp.logical_not(early))
            def _():
                for move in send_c(j, 1):
                    move.wait_send()

            for slot in range(6):
                move_h(j, z, slot, mate).wait_send()

        @pl.when(outer)
        def _():
            move_a(j, z, 0, hub).wait_send()

            @pl.when(early)
            def _():
                for move in rise_c(j):
                    move.wait_send()

        for d in range(1, 2 * n):
            send_t(j, d).wait_send()
        return 0

    with jax.named_scope("drain"):
        lax.fori_loop(0, K, drain, 0)


def fused(mesh, acts_a, acts_b, whiten_a, whiten_b):
    n, m = lax.axis_size("col"), lax.axis_size("tok")
    T, W = acts_a.shape
    V = acts_b.shape[1]
    K = W // LANES
    H = V // 2
    bf, f32 = jnp.bfloat16, jnp.float32
    half = LANES // 2
    units = max(EARLY, 2 * (K - EARLY))
    dma = pltpu.SemaphoreType.DMA
    flops = 2 * (n * W * T * 2 * V + K * half * n * V * V + n * W * W * V // 2)
    total = pl.pallas_call(
        kernel,
        out_shape=jax.ShapeDtypeStruct((W, H), f32),
        in_specs=[pl.BlockSpec(memory_space=pl.ANY)] * 4,
        out_specs=pl.BlockSpec(memory_space=pltpu.VMEM),
        scratch_shapes=[
            pltpu.VMEM((2, T, LANES), bf),
            pltpu.VMEM((K, n, LANES, T), bf),
            pltpu.VMEM((2, T, V), bf),
            pltpu.VMEM((2, n, LANES, H), f32),
            pltpu.VMEM((2, n, LANES, H), f32),
            pltpu.VMEM((2, 2, n, LANES, H), f32),
            pltpu.VMEM((units, n, LANES, H), bf),
            pltpu.VMEM((units, n - 1, LANES, H), bf),
            pltpu.VMEM((units, LANES, H), f32),
            pltpu.VMEM((K, 2, 2, half, H), bf),
            pltpu.VMEM((K, n, 2, half, H), bf),
            pltpu.VMEM((2, n * V, V), bf),
            pltpu.VMEM((K, W, n * LANES), bf),
            pltpu.VMEM((2, LANES, W), bf),
            pltpu.VMEM((K, n, 2, half, H), bf),
            pltpu.VMEM((K, m, half, H), bf),
            dma((2,)), dma, dma((PIECES,)), dma((PIECES,)), dma, dma((PARTS, 4 + n)), dma((2 * n, PARTS)), dma((2,)),
            dma((5, K)), dma((n, K)), dma((2,)), dma((2, 2)), dma((units, n - 1)), dma((units, n - 1)), dma((K, 3, 3)), dma((K, n, 2)),
            dma((K, 6)), dma((K, n)), dma((K, m - 1)), dma((K, m - 1)),
        ],
        compiler_params=pltpu.CompilerParams(collective_id=0, has_side_effects=True, vmem_limit_bytes=67_000_000),
        cost_estimate=pl.CostEstimate(flops=flops, bytes_accessed=2 * (T * (W + V) + n * (W * W + V * V)), transcendentals=0),
    )(acts_a, acts_b, whiten_a, whiten_b)
    return total * (1.0 / jnp.sqrt(jnp.float32(T * m)))


def solution(mesh):
    placed = (P("tok", "col"), P("tok", "col"), P(None, "col"), P(None, "col"))

    def whole(acts_a, acts_b, whiten_a, whiten_b):
        form = functools.partial(fused, mesh) if eligible(mesh, acts_a, acts_b) else body
        return jax.shard_map(form, mesh=mesh, in_specs=placed, out_specs=P("col", "tok"), check_vma=False)(
            acts_a, acts_b, whiten_a, whiten_b)

    return whole
```
